32 devices in a mesh: dp: 4 (over z), mp: 8 (over y, x, core).
Axes of the slice: x: 2, y: 2, z: 4, core: 2. Of those that a mesh axis runs over, the one named last changes fastest.
Arguments:
- policy_hidden: bfloat16 [256, 3584], P('dp'), may hold values from -96 to 96
- reference_hidden: bfloat16 [256, 3584], P('dp'), may hold values from -96 to 96
- policy_gain: float32 [3584], replicated, may hold values from 0.5 to 1.5
- reference_gain: float32 [3584], replicated, may hold values from 0.5 to 1.5
- policy_embedding: bfloat16 [131072, 3584], P(('dp', 'mp')), may hold values from -1 to 1
- reference_embedding: bfloat16 [131072, 3584], P(('dp', 'mp')), may hold values from -1 to 1
- mixture_weight: float32 [256], replicated, may hold values from 0.1 to 0.9
- sampled_tokens: int32 [256], replicated, may hold values from 0 to 131071
Outputs:
- mixture_shift: float32 [256, 131072], P(None, ('dp', 'mp'))
- sampled_logprobs: float32 [3, 256], P(None, 'dp')
The draws below stay inside these ranges and needn't reach their ends.
All inputs are finite; a program needn't handle non-finite values.
Results may differ from the reference program's by a relative error of at most 0.002.
Values may be sent and summed in bfloat16 or wider, within the bound.
A program may use at most 128 MiB of HBM per device.

```python
import math
import jax
import jax.numpy as jnp
from jax import lax

D = 3584
VOCAB = 131072
BATCH = 256


def hidden_states(key):
    keys = jax.random.split(key, 3)
    rows = jnp.exp(jax.random.uniform(keys[1], (BATCH, 1), jnp.float32, 0.0, math.log(10.0)))
    columns = jnp.exp(jax.random.uniform(keys[2], (1, D), jnp.float32, -1.15, 1.15))
    base = jax.random.normal(keys[0], (BATCH, D), jnp.float32)
    return jnp.clip(base * rows * columns, -96.0, 96.0).astype(jnp.bfloat16)


def embedding_rows(key):
    keys = jax.random.split(key, 2)
    place = jnp.arange(VOCAB, dtype=jnp.float32)[:, None] / VOCAB
    jitter = jnp.exp(jax.random.uniform(keys[1], (VOCAB, 1), jnp.float32, -0.5, 0.5))
    scale = 4.0 / math.sqrt(D) * (0.6 + 1.2 * place) * jitter
    base = jax.random.normal(keys[0], (VOCAB, D), jnp.float32)
    return jnp.clip(base * scale, -1.0, 1.0).astype(jnp.bfloat16)


def draw_policy_hidden(key, part):
    return hidden_states(jax.random.fold_in(key, 11))


def draw_reference_hidden(key, part):
    return hidden_states(jax.random.fold_in(key, 12))


def draw_policy_embedding(key, part):
    return embedding_rows(jax.random.fold_in(key, 21))


def draw_reference_embedding(key, part):
    return embedding_rows(jax.random.fold_in(key, 22))


def plant(array, own_key, least, high):
    extent = array.shape
    index_at = [jax.random.randint(jax.random.fold_in(own_key, axis), (), 0, extent[axis]) for axis in range(len(extent))]
    array = array.at[tuple(index_at)].set(least)
    longest = extent.index(max(extent))
    index_at[longest] = (index_at[longest] + 1) % extent[longest]
    return array.at[tuple(index_at)].set(high)


def setup_inputs(seed: int = 0) -> dict:
    key_of = jax.random.split(jax.random.key(seed), 9)
    return {
        "policy_hidden": draw_policy_hidden(jax.random.fold_in(key_of[8], 71), 0),
        "reference_hidden": draw_reference_hidden(jax.random.fold_in(key_of[8], 71), 0),
        "policy_gain": jnp.clip(1.0 + 0.1 * jax.random.normal(key_of[2], (D,), jnp.float32), 0.5, 1.5),
        "reference_gain": jnp.clip(1.0 + 0.1 * jax.random.normal(key_of[3], (D,), jnp.float32), 0.5, 1.5),
        "policy_embedding": draw_policy_embedding(jax.random.fold_in(key_of[8], 71), 0),
        "reference_embedding": draw_reference_embedding(jax.random.fold_in(key_of[8], 71), 0),
        "mixture_weight": jnp.clip(jax.random.uniform(key_of[6], (BATCH,), jnp.float32, 0.1, 0.9), 0.1, 0.9),
        "sampled_tokens": plant(jax.random.randint(key_of[7], (BATCH,), 0, VOCAB), jax.random.fold_in(key_of[7], 1), 0, VOCAB - 1).astype(jnp.int32),
    }


softcap = 30.0
epsilon = 1e-06

def normalize(hidden, gain):
    values = hidden.astype(jnp.float32)
    meansq = lax.optimization_barrier(jnp.mean(values * values, axis=-1, keepdims=True))
    return (values * lax.rsqrt(meansq + epsilon) * gain).astype(jnp.bfloat16)

def project(normed, embedding):
    raw = lax.dot_general(normed, embedding, (((1,), (1,)), ((), ())), preferred_element_type=jnp.float32)
    return softcap * jnp.tanh(raw / softcap)

def reference(policy_hidden, reference_hidden, policy_gain, reference_gain, policy_embedding, reference_embedding, mixture_weight, sampled_tokens):
    capped_policy = project(normalize(policy_hidden, policy_gain), policy_embedding)
    capped_reference = project(normalize(reference_hidden, reference_gain), reference_embedding)
    weight = mixture_weight[:, None]
    mixed = (1.0 - weight) * capped_policy + weight * capped_reference
    policy_total = jnp.log(lax.optimization_barrier(jnp.sum(jnp.exp(capped_policy), axis=1)))
    reference_total = jnp.log(lax.optimization_barrier(jnp.sum(jnp.exp(capped_reference), axis=1)))
    mixture_total = jnp.log(lax.optimization_barrier(jnp.sum(jnp.exp(mixed), axis=1)))
    mixture_shift = mixed - mixture_total[:, None] - (capped_policy - policy_total[:, None])
    chosen = sampled_tokens.astype(jnp.int32)[:, None]
    policy_pick = jnp.take_along_axis(capped_policy, chosen, axis=1)[:, 0]
    reference_pick = jnp.take_along_axis(capped_reference, chosen, axis=1)[:, 0]
    mixed_pick = (1.0 - mixture_weight) * policy_pick + mixture_weight * reference_pick
    sampled_logprobs = jnp.stack([policy_pick - policy_total, reference_pick - reference_total, mixed_pick - mixture_total])
    return (mixture_shift, sampled_logprobs)
```

```python
import functools

import jax
import jax.numpy as jnp
from jax import lax
from jax.experimental import pallas as pl
from jax.experimental.pallas import tpu as pltpu
from jax.sharding import PartitionSpec as P

softcap = 30.0
epsilon = 1e-06
LANES = 128
TILE = 512
SLOT_BYTES = 40 * 2**20
MESH = pl.DeviceIdType.MESH


def lane_sum(x):
    total = x[:, :LANES]
    for k in range(1, x.shape[1] // LANES):
        total = total + x[:, k * LANES : (k + 1) * LANES]
    return total


def spread(row, lanes):
    return jnp.transpose(jnp.broadcast_to(row, (LANES, row.shape[1])))[:, :lanes]


def kernel(
    n_dp,
    n_mp,
    tile,
    slots,
    ph_hbm,
    rh_hbm,
    pg_hbm,
    rg_hbm,
    pe_hbm,
    re_hbm,
    weight_ref,
    token_ref,
    diff_hbm,
    delta_ref,
    logp_ref,
    hidden,
    gains,
    normed,
    emb,
    diff,
    sums,
    weight_col,
    token_col,
    part_mp,
    part_dp,
    in_sem,
    emb_sem,
    out_sem,
    send_sem,
    recv_sem,
    fsend_sem,
    frecv_sem,
    msend_sem,
    mrecv_sem,
    dsend_sem,
    drecv_sem,
):
    dp = lax.axis_index("dp")
    mp = lax.axis_index("mp")
    half = lax.rem(mp, 2)
    partner = mp + 1 - 2 * half
    seq = hidden.shape[1]
    rows = seq // 2
    batch = normed.shape[1]
    vocab = pe_hbm.shape[0]
    tiles = vocab // tile

    loads = [
        pltpu.make_async_copy(ph_hbm, hidden.at[0], in_sem.at[0]),
        pltpu.make_async_copy(pg_hbm, gains.at[0], in_sem.at[1]),
        pltpu.make_async_copy(rh_hbm, hidden.at[1], in_sem.at[2]),
        pltpu.make_async_copy(rg_hbm, gains.at[1], in_sem.at[3]),
    ]
    for load in loads:
        load.start()

    def fetch(source, t, slot):
        return pltpu.make_async_copy(
            source.at[pl.ds(pl.multiple_of(t * tile, tile), tile)], emb.at[slot], emb_sem.at[slot]
        )

    for g in range(slots):
        fetch(pe_hbm if g < tiles else re_hbm, g % tiles, g).start()

    barrier = pltpu.get_barrier_semaphore()
    for o in range(1, n_dp):
        pl.semaphore_signal(
            barrier, inc=1, device_id={"dp": lax.rem(dp + o, n_dp)}, device_id_type=MESH
        )
    for o in range(1, n_mp):
        pl.semaphore_signal(
            barrier, inc=1, device_id={"mp": lax.rem(mp + o, n_mp)}, device_id_type=MESH
        )

    def normalize(model):
        loads[2 * model].wait()
        loads[2 * model + 1].wait()
        for r in range(0, seq, 16):
            values = hidden[model, r : r + 16].astype(jnp.float32)
            meansq = jnp.mean(values * values, axis=-1, keepdims=True)
            result = (values * lax.rsqrt(meansq + epsilon) * gains[model]).astype(jnp.bfloat16)
            normed[model, pl.ds(pl.multiple_of(dp * seq + r, 16), 16)] = result

    def my_half(model, owner):
        return normed.at[model, pl.ds(pl.multiple_of(owner * seq + half * rows, rows), rows)]

    def other_half(model, owner):
        return normed.at[
            model, pl.ds(pl.multiple_of(owner * seq + (1 - half) * rows, rows), rows)
        ]

    offsets = sorted(range(1, n_dp), key=lambda o: min(o, n_dp - o))

    def gather_copy(model, o):
        return pltpu.make_async_remote_copy(
            src_ref=my_half(model, dp),
            dst_ref=my_half(model, dp),
            send_sem=send_sem.at[model, o],
            recv_sem=recv_sem.at[model, o],
            device_id={"dp": lax.rem(dp + o, n_dp)},
            device_id_type=MESH,
        )

    def arrived(model, o):
        owner = lax.rem(dp + n_dp - o, n_dp)
        return pltpu.make_async_remote_copy(
            src_ref=my_half(model, owner),
            dst_ref=my_half(model, owner),
            send_sem=send_sem.at[model, o],
            recv_sem=recv_sem.at[model, o],
            device_id={"dp": lax.rem(dp + o, n_dp)},
            device_id_type=MESH,
        )

    def forward(model, o, part):
        owner = lax.rem(dp + n_dp - o, n_dp)
        return pltpu.make_async_remote_copy(
            src_ref=part(model, owner),
            dst_ref=part(model, owner),
            send_sem=fsend_sem.at[model, o],
            recv_sem=frecv_sem.at[model, o],
            device_id={"mp": partner},
            device_id_type=MESH,
        )

    normalize(0)
    pl.semaphore_wait(barrier, n_dp - 1 + n_mp - 1)
    for o in offsets:
        gather_copy(0, o).start()
    normalize(1)
    for o in offsets:
        gather_copy(1, o).start()

    first = (dp * n_mp + mp) * vocab
    weight = weight_ref[...]
    weight_col[...] = spread(weight, LANES)
    local_token = jnp.clip(token_ref[...] - first, -1, vocab).astype(jnp.float32)
    token_col[...] = spread(local_token, LANES)
    sums[...] = jnp.zeros_like(sums)

    def relay(model):
        for o in offsets:
            arrived(model, o).wait_recv()
            forward(model, o, my_half).start()

    def relayed(model):
        for o in offsets:
            forward(model, o, other_half).wait_recv()

    def project(model, slot):
        raw = lax.dot_general(
            normed[model],
            emb[slot],
            (((1,), (1,)), ((), ())),
            preferred_element_type=jnp.float32,
        )
        return softcap * jnp.tanh(raw * (1.0 / softcap))

    def picked(t, values):
        total = None
        lane = lax.broadcasted_iota(jnp.int32, (batch, LANES), 1)
        token = token_col[...]
        for k in range(tile // LANES):
            column = (lane + (t * tile + k * LANES)).astype(jnp.float32)
            piece = jnp.where(token == column, values[:, k * LANES : (k + 1) * LANES], 0.0)
            total = piece if total is None else total + piece
        return total

    def columns(t):
        return pl.ds(pl.multiple_of(t * tile, tile), tile)

    relay(0)
    relayed(0)

    @pl.loop(0, tiles)
    def _(t):
        slot = lax.rem(t, slots)
        fetch(pe_hbm, t, slot).wait()
        capped = project(0, slot)
        diff[:, columns(t)] = capped
        sums[0] += lane_sum(jnp.exp(capped))
        sums[3] += picked(t, capped)
        later = t + slots

        @pl.when(later < tiles)
        def _():
            fetch(pe_hbm, later, slot).start()

        @pl.when(jnp.logical_and(later >= tiles, later < 2 * tiles))
        def _():
            fetch(re_hbm, later - tiles, slot).start()

    relay(1)
    relayed(1)

    def put(t):
        return pltpu.make_async_copy(diff.at[:, columns(t)], diff_hbm.at[:, columns(t)], out_sem.at[t])

    @pl.loop(0, tiles)
    def _(t):
        g = t + tiles
        slot = lax.rem(g, slots)
        fetch(re_hbm, t, slot).wait()
        capped = project(1, slot)
        policy = diff[:, columns(t)]
        w = jnp.concatenate([weight_col[...]] * (tile // LANES), axis=1)
        mixed = (1.0 - w) * policy + w * capped
        diff[:, columns(t)] = mixed - policy
        put(t).start()
        sums[1] += lane_sum(jnp.exp(capped))
        sums[2] += lane_sum(jnp.exp(mixed))
        sums[4] += picked(t, capped)
        later = g + slots

        @pl.when(later < 2 * tiles)
        def _():
            fetch(re_hbm, later - tiles, slot).start()

    lane = lax.broadcasted_iota(jnp.int32, (batch, LANES), 1)
    packed = jnp.zeros((batch, LANES), jnp.float32)
    for k in range(5):
        packed = jnp.where(lane == k, jnp.sum(sums[k], axis=1, keepdims=True), packed)
    part_mp[0] = jnp.transpose(packed)[:8]

    def share(buffer, axis, me, n, o, send, recv):
        return pltpu.make_async_remote_copy(
            src_ref=buffer.at[0],
            dst_ref=buffer.at[o],
            send_sem=send.at[o],
            recv_sem=recv.at[o],
            device_id={axis: lax.rem(me + o, n)},
            device_id_type=MESH,
        )

    def reduce(buffer, axis, me, n, send, recv):
        for o in range(1, n):
            share(buffer, axis, me, n, o, send, recv).start()
        for o in range(1, n):
            share(buffer, axis, me, n, o, send, recv).wait_recv()
        total = buffer[0]
        for o in range(1, n):
            total = total + buffer[o]
        return total

    part_dp[0] = reduce(part_mp, "mp", mp, n_mp, msend_sem, mrecv_sem)
    total = reduce(part_dp, "dp", dp, n_dp, dsend_sem, drecv_sem)
    policy_total = jnp.log(total[0:1])
    reference_total = jnp.log(total[1:2])
    mixture_total = jnp.log(total[2:3])
    policy_pick = total[3:4]
    reference_pick = total[4:5]
    mixed_pick = (1.0 - weight) * policy_pick + weight * reference_pick
    logp_ref[0:1] = policy_pick - policy_total
    logp_ref[1:2] = reference_pick - reference_total
    logp_ref[2:3] = mixed_pick - mixture_total
    delta_ref[...] = spread(mixture_total - policy_total, LANES)

    @pl.loop(0, tiles)
    def _(t):
        put(t).wait()

    for model in range(2):
        for o in offsets:
            gather_copy(model, o).wait_send()
            forward(model, o, my_half).wait_send()
    for o in range(1, n_mp):
        share(part_mp, "mp", mp, n_mp, o, msend_sem, mrecv_sem).wait_send()
    for o in range(1, n_dp):
        share(part_dp, "dp", dp, n_dp, o, dsend_sem, drecv_sem).wait_send()


def local(
    n_dp,
    n_mp,
    policy_hidden,
    reference_hidden,
    policy_gain,
    reference_gain,
    policy_embedding,
    reference_embedding,
    mixture_weight,
    sampled_tokens,
):
    seq, width = policy_hidden.shape
    vocab = policy_embedding.shape[0]
    batch = mixture_weight.shape[0]
    tile = min(TILE, vocab)
    tiles = vocab // tile
    slots = min(2 * tiles, SLOT_BYTES // (tile * width * 2))
    anywhere = pl.BlockSpec(memory_space=pl.ANY)
    vmem = pl.BlockSpec(memory_space=pltpu.VMEM)
    dma = pltpu.SemaphoreType.DMA
    diff, delta, logp = pl.pallas_call(
        functools.partial(kernel, n_dp, n_mp, tile, slots),
        name="mixture",
        out_shape=(
            jax.ShapeDtypeStruct((batch, vocab), jnp.float32),
            jax.ShapeDtypeStruct((batch, LANES), jnp.float32),
            jax.ShapeDtypeStruct((3, batch), jnp.float32),
        ),
        in_specs=[anywhere] * 6 + [vmem] * 2,
        out_specs=(anywhere, vmem, vmem),
        scratch_shapes=[
            pltpu.VMEM((2, seq, width), jnp.bfloat16),
            pltpu.VMEM((2, 1, width), jnp.float32),
            pltpu.VMEM((2, batch, width), jnp.bfloat16),
            pltpu.VMEM((slots, tile, width), jnp.bfloat16),
            pltpu.VMEM((batch, vocab), jnp.float32),
            pltpu.VMEM((5, batch, LANES), jnp.float32),
            pltpu.VMEM((batch, LANES), jnp.float32),
            pltpu.VMEM((batch, LANES), jnp.float32),
            pltpu.VMEM((n_mp, 8, batch), jnp.float32),
            pltpu.VMEM((n_dp, 8, batch), jnp.float32),
            dma((4,)),
            dma((slots,)),
            dma((tiles,)),
            dma((2, n_dp)),
            dma((2, n_dp)),
            dma((2, n_dp)),
            dma((2, n_dp)),
            dma((n_mp,)),
            dma((n_mp,)),
            dma((n_dp,)),
            dma((n_dp,)),
        ],
        compiler_params=pltpu.CompilerParams(
            collective_id=0, has_side_effects=True, vmem_limit_bytes=57 * 2**20
        ),
    )(
        policy_hidden,
        reference_hidden,
        policy_gain.reshape(1, width),
        reference_gain.reshape(1, width),
        policy_embedding,
        reference_embedding,
        mixture_weight.reshape(1, batch),
        sampled_tokens.reshape(1, batch),
    )
    mixture_shift = diff - delta[:, :1]
    sampled_logprobs = lax.dynamic_slice_in_dim(logp, lax.axis_index("dp") * seq, seq, 1)
    return (mixture_shift, sampled_logprobs)


def solution(mesh):
    in_specs = (
        P("dp", None),
        P("dp", None),
        P(),
        P(),
        P(("dp", "mp"), None),
        P(("dp", "mp"), None),
        P(),
        P(),
    )
    out_specs = (P(None, ("dp", "mp")), P(None, "dp"))
    body = functools.partial(local, mesh.shape["dp"], mesh.shape["mp"])
    return jax.shard_map(body, mesh=mesh, in_specs=in_specs, out_specs=out_specs, check_vma=False)
```

```python
import functools

import jax
import jax.numpy as jnp
from jax import lax
from jax.experimental import pallas as pl
from jax.experimental.pallas import tpu as pltpu
from jax.sharding import PartitionSpec as P

softcap = 30.0
epsilon = 1e-06
LANES = 128
TILE = 512
SLOT_BYTES = 40 * 2**20
MESH = pl.DeviceIdType.MESH


def lane_sum(x):
    total = x[:, :LANES]
    for k in range(1, x.shape[1] // LANES):
        total = total + x[:, k * LANES : (k + 1) * LANES]
    return total


def spread(row, lanes):
    return jnp.transpose(jnp.broadcast_to(row, (LANES, row.shape[1])))[:, :lanes]


def kernel(
    n_dp,
    n_mp,
    tile,
    slots,
    ph_hbm,
    rh_hbm,
    pg_hbm,
    rg_hbm,
    pe_hbm,
    re_hbm,
    weight_ref,
    token_ref,
    diff_hbm,
    delta_ref,
    logp_ref,
    hidden,
    gains,
    normed,
    emb,
    diff,
    sums,
    weight_col,
    token_col,
    part_mp,
    part_dp,
    in_sem,
    emb_sem,
    out_sem,
    send_sem,
    recv_sem,
    fsend_sem,
    frecv_sem,
    psend_sem,
    precv_sem,
    msend_sem,
    mrecv_sem,
    dsend_sem,
    drecv_sem,
):
    dp = lax.axis_index("dp")
    mp = lax.axis_index("mp")
    half = lax.rem(mp, 2)
    seq = hidden.shape[1]
    group = 2 * (seq // 16)
    width = hidden.shape[2] // 2
    me = lax.rem(mp, group)
    base = mp - me
    twin = me + 1 - 2 * half
    hops = range(2, group, 2)
    batch = normed.shape[1]
    vocab = pe_hbm.shape[0]
    tiles = vocab // tile

    loads = [
        pltpu.make_async_copy(ph_hbm, hidden.at[0], in_sem.at[0]),
        pltpu.make_async_copy(pg_hbm, gains.at[0], in_sem.at[1]),
        pltpu.make_async_copy(rh_hbm, hidden.at[1], in_sem.at[2]),
        pltpu.make_async_copy(rg_hbm, gains.at[1], in_sem.at[3]),
    ]
    for load in loads:
        load.start()

    def fetch(source, t, slot):
        return pltpu.make_async_copy(
            source.at[pl.ds(pl.multiple_of(t * tile, tile), tile)], emb.at[slot], emb_sem.at[slot]
        )

    for g in range(slots):
        fetch(pe_hbm if g < tiles else re_hbm, g % tiles, g).start()

    barrier = pltpu.get_barrier_semaphore()
    for o in range(1, n_dp):
        pl.semaphore_signal(
            barrier, inc=1, device_id={"dp": lax.rem(dp + o, n_dp)}, device_id_type=MESH
        )
    for o in range(1, n_mp):
        pl.semaphore_signal(
            barrier, inc=1, device_id={"mp": lax.rem(mp + o, n_mp)}, device_id_type=MESH
        )

    def normalize(model):
        loads[2 * model].wait()
        loads[2 * model + 1].wait()
        for r in range(0, seq, 16):
            values = hidden[model, r : r + 16].astype(jnp.float32)
            meansq = jnp.mean(values * values, axis=-1, keepdims=True)
            result = (values * lax.rsqrt(meansq + epsilon) * gains[model]).astype(jnp.bfloat16)
            normed[model, pl.ds(pl.multiple_of(dp * seq + r, 16), 16)] = result

    def block(model, owner, member):
        row = pl.multiple_of(owner * seq + member // 2 * 16, 16)
        column = pl.multiple_of(lax.rem(member, 2) * width, 128)
        return normed.at[model, pl.ds(row, 16), pl.ds(column, width)]

    offsets = sorted(range(1, n_dp), key=lambda o: min(o, n_dp - o))

    def gather_copy(model, o):
        return pltpu.make_async_remote_copy(
            src_ref=block(model, dp, me),
            dst_ref=block(model, dp, me),
            send_sem=send_sem.at[model, o],
            recv_sem=recv_sem.at[model, o],
            device_id={"dp": lax.rem(dp + o, n_dp)},
            device_id_type=MESH,
        )

    def arrived(model, o):
        owner = lax.rem(dp + n_dp - o, n_dp)
        return pltpu.make_async_remote_copy(
            src_ref=block(model, owner, me),
            dst_ref=block(model, owner, me),
            send_sem=send_sem.at[model, o],
            recv_sem=recv_sem.at[model, o],
            device_id={"dp": lax.rem(dp + o, n_dp)},
            device_id_type=MESH,
        )

    def member_of(index, q):
        return lax.rem(index + group - q, group)

    def pass_on(model, o, q, member):
        owner = lax.rem(dp + n_dp - o, n_dp)
        return pltpu.make_async_remote_copy(
            src_ref=block(model, owner, member),
            dst_ref=block(model, owner, member),
            send_sem=psend_sem.at[model, o, q],
            recv_sem=precv_sem.at[model, o, q],
            device_id={"mp": base + lax.rem(me + q, group)},
            device_id_type=MESH,
        )

    def forward(model, o, q, member):
        owner = lax.rem(dp + n_dp - o, n_dp)
        return pltpu.make_async_remote_copy(
            src_ref=block(model, owner, member),
            dst_ref=block(model, owner, member),
            send_sem=fsend_sem.at[model, o, q],
            recv_sem=frecv_sem.at[model, o, q],
            device_id={"mp": base + twin},
            device_id_type=MESH,
        )

    normalize(0)
    pl.semaphore_wait(barrier, n_dp - 1 + n_mp - 1)
    for o in offsets:
        gather_copy(0, o).start()
    normalize(1)
    for o in offsets:
        gather_copy(1, o).start()

    first = (dp * n_mp + mp) * vocab
    weight = weight_ref[...]
    weight_col[...] = spread(weight, LANES)
    local_token = jnp.clip(token_ref[...] - first, -1, vocab).astype(jnp.float32)
    token_col[...] = spread(local_token, LANES)
    sums[...] = jnp.zeros_like(sums)

    def relay(model):
        for o in offsets:
            arrived(model, o).wait_recv()
            for q in hops:
                pass_on(model, o, q, me).start()
            forward(model, o, 0, me).start()
        for o in offsets:
            for q in hops:
                member = member_of(me, q)
                pass_on(model, o, q, member).wait_recv()
                forward(model, o, q, member).start()

    def relayed(model):
        for o in offsets:
            for q in range(0, group, 2):
                forward(model, o, q, member_of(twin, q)).wait_recv()

    def project(model, slot):
        raw = lax.dot_general(
            normed[model],
            emb[slot],
            (((1,), (1,)), ((), ())),
            preferred_element_type=jnp.float32,
        )
        return softcap * jnp.tanh(raw * (1.0 / softcap))

    def picked(t, values):
        total = None
        lane = lax.broadcasted_iota(jnp.int32, (batch, LANES), 1)
        token = token_col[...]
        for k in range(tile // LANES):
            column = (lane + (t * tile + k * LANES)).astype(jnp.float32)
            piece = jnp.where(token == column, values[:, k * LANES : (k + 1) * LANES], 0.0)
            total = piece if total is None else total + piece
        return total

    def columns(t):
        return pl.ds(pl.multiple_of(t * tile, tile), tile)

    relay(0)
    relayed(0)

    @pl.loop(0, tiles)
    def _(t):
        slot = lax.rem(t, slots)
        fetch(pe_hbm, t, slot).wait()
        capped = project(0, slot)
        diff[:, columns(t)] = capped
        sums[0] += lane_sum(jnp.exp(capped))
        sums[3] += picked(t, capped)
        later = t + slots

        @pl.when(later < tiles)
        def _():
            fetch(pe_hbm, later, slot).start()

        @pl.when(jnp.logical_and(later >= tiles, later < 2 * tiles))
        def _():
            fetch(re_hbm, later - tiles, slot).start()

    relay(1)
    relayed(1)

    def put(t):
        return pltpu.make_async_copy(diff.at[:, columns(t)], diff_hbm.at[:, columns(t)], out_sem.at[t])

    @pl.loop(0, tiles)
    def _(t):
        g = t + tiles
        slot = lax.rem(g, slots)
        fetch(re_hbm, t, slot).wait()
        capped = project(1, slot)
        policy = diff[:, columns(t)]
        w = jnp.concatenate([weight_col[...]] * (tile // LANES), axis=1)
        mixed = (1.0 - w) * policy + w * capped
        diff[:, columns(t)] = mixed - policy
        put(t).start()
        sums[1] += lane_sum(jnp.exp(capped))
        sums[2] += lane_sum(jnp.exp(mixed))
        sums[4] += picked(t, capped)
        later = g + slots

        @pl.when(later < 2 * tiles)
        def _():
            fetch(re_hbm, later - tiles, slot).start()

    lane = lax.broadcasted_iota(jnp.int32, (batch, LANES), 1)
    packed = jnp.zeros((batch, LANES), jnp.float32)
    for k in range(5):
        packed = jnp.where(lane == k, jnp.sum(sums[k], axis=1, keepdims=True), packed)
    part_mp[0] = jnp.transpose(packed)[:8]

    def share(buffer, axis, me, n, o, send, recv):
        return pltpu.make_async_remote_copy(
            src_ref=buffer.at[0],
            dst_ref=buffer.at[o],
            send_sem=send.at[o],
            recv_sem=recv.at[o],
            device_id={axis: lax.rem(me + o, n)},
            device_id_type=MESH,
        )

    def reduce(buffer, axis, me, n, send, recv):
        for o in range(1, n):
            share(buffer, axis, me, n, o, send, recv).start()
        for o in range(1, n):
            share(buffer, axis, me, n, o, send, recv).wait_recv()
        total = buffer[0]
        for o in range(1, n):
            total = total + buffer[o]
        return total

    part_dp[0] = reduce(part_mp, "mp", mp, n_mp, msend_sem, mrecv_sem)
    total = reduce(part_dp, "dp", dp, n_dp, dsend_sem, drecv_sem)
    policy_total = jnp.log(total[0:1])
    reference_total = jnp.log(total[1:2])
    mixture_total = jnp.log(total[2:3])
    policy_pick = total[3:4]
    reference_pick = total[4:5]
    mixed_pick = (1.0 - weight) * policy_pick + weight * reference_pick
    logp = (policy_pick - policy_total, reference_pick - reference_total, mixed_pick - mixture_total)
    for k, row in enumerate(logp):
        mine = row[:, :seq]
        for owner in range(1, n_dp):
            mine = jnp.where(dp == owner, row[:, owner * seq : (owner + 1) * seq], mine)
        logp_ref[k : k + 1] = mine
    delta_ref[...] = spread(mixture_total - policy_total, LANES)

    @pl.loop(0, tiles)
    def _(t):
        put(t).wait()

    for model in range(2):
        for o in offsets:
            gather_copy(model, o).wait_send()
            for q in hops:
                pass_on(model, o, q, me).wait_send()
            for q in range(0, group, 2):
                forward(model, o, q, member_of(me, q)).wait_send()
    for o in range(1, n_mp):
        share(part_mp, "mp", mp, n_mp, o, msend_sem, mrecv_sem).wait_send()
    for o in range(1, n_dp):
        share(part_dp, "dp", dp, n_dp, o, dsend_sem, drecv_sem).wait_send()


def local(
    n_dp,
    n_mp,
    policy_hidden,
    reference_hidden,
    policy_gain,
    reference_gain,
    policy_embedding,
    reference_embedding,
    mixture_weight,
    sampled_tokens,
):
    seq, width = policy_hidden.shape
    vocab = policy_embedding.shape[0]
    batch = mixture_weight.shape[0]
    tile = min(TILE, vocab)
    tiles = vocab // tile
    slots = min(2 * tiles, SLOT_BYTES // (tile * width * 2))
    group = 2 * (seq // 16)
    anywhere = pl.BlockSpec(memory_space=pl.ANY)
    vmem = pl.BlockSpec(memory_space=pltpu.VMEM)
    dma = pltpu.SemaphoreType.DMA
    diff, delta, logp = pl.pallas_call(
        functools.partial(kernel, n_dp, n_mp, tile, slots),
        name="mixture",
        out_shape=(
            jax.ShapeDtypeStruct((batch, vocab), jnp.float32),
            jax.ShapeDtypeStruct((batch, LANES), jnp.float32),
            jax.ShapeDtypeStruct((3, seq), jnp.float32),
        ),
        in_specs=[anywhere] * 6 + [vmem] * 2,
        out_specs=(anywhere, vmem, vmem),
        scratch_shapes=[
            pltpu.VMEM((2, seq, width), jnp.bfloat16),
            pltpu.VMEM((2, 1, width), jnp.float32),
            pltpu.VMEM((2, batch, width), jnp.bfloat16),
            pltpu.VMEM((slots, tile, width), jnp.bfloat16),
            pltpu.VMEM((batch, vocab), jnp.float32),
            pltpu.VMEM((5, batch, LANES), jnp.float32),
            pltpu.VMEM((batch, LANES), jnp.float32),
            pltpu.VMEM((batch, LANES), jnp.float32),
            pltpu.VMEM((n_mp, 8, batch), jnp.float32),
            pltpu.VMEM((n_dp, 8, batch), jnp.float32),
            dma((4,)),
            dma((slots,)),
            dma((tiles,)),
            dma((2, n_dp)),
            dma((2, n_dp)),
            dma((2, n_dp, group)),
            dma((2, n_dp, group)),
            dma((2, n_dp, group)),
            dma((2, n_dp, group)),
            dma((n_mp,)),
            dma((n_mp,)),
            dma((n_dp,)),
            dma((n_dp,)),
        ],
        compiler_params=pltpu.CompilerParams(
            collective_id=0, has_side_effects=True, vmem_limit_bytes=57 * 2**20
        ),
    )(
        policy_hidden,
        reference_hidden,
        policy_gain.reshape(1, width),
        reference_gain.reshape(1, width),
        policy_embedding,
        reference_embedding,
        mixture_weight.reshape(1, batch),
        sampled_tokens.reshape(1, batch),
    )
    mixture_shift = diff - delta[:, :1]
    return (mixture_shift, logp)


def solution(mesh):
    in_specs = (
        P("dp", None),
        P("dp", None),
        P(),
        P(),
        P(("dp", "mp"), None),
        P(("dp", "mp"), None),
        P(),
        P(),
    )
    out_specs = (P(None, ("dp", "mp")), P(None, "dp"))
    body = functools.partial(local, mesh.shape["dp"], mesh.shape["mp"])
    return jax.shard_map(body, mesh=mesh, in_specs=in_specs, out_specs=out_specs, check_vma=False)
```
